1024 devices in a mesh: gx: 128 (over z, y), gy: 8 (over x, core).
Axes of the slice: x: 4, y: 4, z: 32, core: 2. Of those that a mesh axis runs over, the one named last changes fastest.
Arguments:
- residual_block: float32 [8, 512, 64, 256], P(None, 'gx', 'gy'), may hold values from -70 to 70
- diagonal: float32 [512, 64, 256], P('gx', 'gy'), may hold values from 0.5 to 4
Outputs:
- correction: float32 [8, 512, 64, 256], P(None, 'gx', 'gy')
- new_residual: float32 [8, 512, 64, 256], P(None, 'gx', 'gy')
- estimate: float32 [8], replicated
The draws below stay inside these ranges and needn't reach their ends.
All inputs are finite; a program needn't handle non-finite values.
Results may differ from the reference program's by a relative error of at most 0.008.
Values sent between devices are 32-bit elements; how exact they have to be, the bound alone decides.
A program may use at most 32 MiB of HBM per device.

```python
import math
import jax
import jax.numpy as jnp
import numpy as np
from jax import lax

NRHS = 8
NX = 512
NY = 64
NZ = 256


def draw_residual_block(key, part):
    third = jax.random.fold_in(jax.random.fold_in(key, 17), 2)
    coord_x = jnp.arange(NX, dtype=jnp.float32) / NX
    rising = jnp.exp(math.log(3.0) * coord_x)[None, :, None, None]
    values = jnp.clip(jax.random.normal(third, (NRHS, NX, NY, NZ), jnp.float32), -4.0, 4.0)
    return (values * rising).astype(jnp.float32)


def level_of(own_key, shape, cuts, low, top_value):
    factor_of, own = 1.0, jax.random.fold_in(own_key, 6)
    for position, shards_of in cuts:
        heights = jnp.exp(jax.random.uniform(jax.random.fold_in(own, position), (shards_of,), jnp.float32, low / len(cuts), top_value / len(cuts)))
        factor_of = factor_of * jnp.repeat(heights, shape[position] // shards_of).reshape([-1 if axis == position else 1 for axis in range(len(shape))])
    return factor_of


def setup_inputs(seed: int = 0) -> dict:
    streams_of = jax.random.split(jax.random.key(seed), 3)
    residual_block = draw_residual_block(jax.random.fold_in(streams_of[2], 71), 0)
    diagonal = jnp.clip(jnp.exp(math.log(4.0) - 2.0794415 * jax.random.uniform(streams_of[1], (NX, NY, NZ), jnp.float32) ** level_of(streams_of[1], (NX, NY, NZ), ((0, 128), (1, 8)), -0.2, 0.2)), 0.5, 4.0)
    return {"residual_block": residual_block, "diagonal": diagonal}


WEIGHT_X = 0.4
WEIGHT_Y = 0.2
WEIGHT_Z = 0.1
CENTRE = 2.2
SCALE_POWER = 3.0
SHIFTS = (6.0, 1.5, 4.5, 3.0)
EPSILON = 1e-06

def apply_padded(padded, diag_inner, shift_now):
    along_z = jnp.pad(padded, ((0, 0), (0, 0), (0, 0), (1, 1)))
    sum_z = padded + WEIGHT_Z * (along_z[..., :-2] + along_z[..., 2:])
    sum_y = sum_z[:, :, 1:-1] + WEIGHT_Y * (sum_z[:, :, :-2] + sum_z[:, :, 2:])
    sum_x = sum_y[:, 1:-1] + WEIGHT_X * (sum_y[:, :-2] + sum_y[:, 2:])
    centre_cells = padded[:, 1:-1, 1:-1]
    return ((CENTRE + 1.0 + diag_inner - shift_now) * centre_cells - sum_x) / SCALE_POWER

def newton_table():
    blocks = len(SHIFTS)
    identity = np.eye(NRHS, dtype=np.float32)
    matrix = np.zeros(((blocks + 1) * NRHS, blocks * NRHS), np.float32)
    for block_index in range(blocks):
        low = block_index * NRHS
        matrix[low:low + NRHS, low:low + NRHS] = SHIFTS[block_index] * identity
        matrix[low + NRHS:low + 2 * NRHS, low:low + NRHS] = SCALE_POWER * identity
    return matrix

def solve_small(gram_full):
    highest = lax.Precision.HIGHEST
    newton = jnp.asarray(newton_table(), gram_full.dtype)
    image = jnp.dot(newton.T, jnp.dot(gram_full, newton, precision=highest), precision=highest)
    right_side = jnp.dot(newton.T, gram_full[:, :NRHS], precision=highest)
    scales = lax.rsqrt(jnp.diagonal(image) + EPSILON)
    scaled = image * scales[:, None] * scales[None, :]
    factor = jnp.linalg.cholesky(scaled)
    coeffs = scales[:, None] * jax.scipy.linalg.cho_solve((factor, True), scales[:, None] * right_side)
    initial_sq = jnp.diagonal(gram_full)[:NRHS]
    estimate = (initial_sq - lax.optimization_barrier(jnp.sum(right_side * coeffs, axis=0))) / initial_sq
    return (coeffs, jnp.dot(newton, coeffs, precision=highest), estimate)

def reference(residual_block, diagonal):
    highest = lax.Precision.HIGHEST
    powers = [residual_block]
    field_now = residual_block
    for shift_now in SHIFTS:
        padded = jnp.pad(field_now, ((0, 0), (1, 1), (1, 1), (0, 0)))
        field_now = apply_padded(padded, diagonal, shift_now)
        powers.append(field_now)
    basis = jnp.concatenate(powers, 0).reshape(len(powers) * NRHS, -1)
    gram_full = lax.dot_general(basis.astype(jnp.float32), basis.astype(jnp.float32), (((1,), (1,)), ((), ())), precision=highest, preferred_element_type=jnp.float32)
    coeffs, combined, estimate = solve_small(gram_full)
    kept = len(SHIFTS) * NRHS
    correction = lax.dot_general(coeffs.astype(jnp.float32), basis[:kept].astype(jnp.float32), (((0,), (0,)), ((), ())), precision=highest, preferred_element_type=jnp.float32)
    removed = lax.dot_general(combined.astype(jnp.float32), basis.astype(jnp.float32), (((0,), (0,)), ((), ())), precision=highest, preferred_element_type=jnp.float32)
    new_residual = residual_block - removed.reshape(residual_block.shape)
    return (correction.reshape(residual_block.shape), new_residual, estimate)
```

```python
import functools

import jax
import jax.numpy as jnp
import numpy as np
from jax import lax
from jax.experimental import pallas as pl
from jax.experimental.pallas import tpu as pltpu
from jax.sharding import PartitionSpec as P

NRHS = 8
GX = "gx"


WEIGHT_X = 0.4
WEIGHT_Y = 0.2
WEIGHT_Z = 0.1
CENTRE = 2.2
SCALE_POWER = 3.0
SHIFTS = (6.0, 1.5, 4.5, 3.0)
EPSILON = 1e-06


def padded_2(block, sides, width):
    for axis, dim in sides:
        count = lax.axis_size(axis)
        forward = [(i, i + 1) for i in range(count - 1)]
        backward = [(target, source) for source, target in forward]
        low = lax.ppermute(
            lax.slice_in_dim(block, block.shape[dim] - width, None, axis=dim), axis, forward
        )
        high = lax.ppermute(lax.slice_in_dim(block, 0, width, axis=dim), axis, backward)
        block = jnp.concatenate([low, block, high], axis=dim)
    return block


def moments_of(gram):
    n = NRHS
    last = len(SHIFTS)
    rows = [gram[:n, j * n : (j + 1) * n] for j in range(last + 1)]
    rows += [gram[last * n :, j * n : (j + 1) * n] for j in range(1, last + 1)]
    flat = jnp.stack(rows).reshape(-1)
    return jnp.pad(flat, (0, ROWS * 128 - flat.shape[0])).reshape(ROWS, 128)


def from_moments(words):
    n, last = NRHS, len(SHIFTS)
    blocks = words.reshape(-1)[: (2 * last + 1) * n * n].reshape(2 * last + 1, n, n)
    table = {(0, j): blocks[j] for j in range(last + 1)}
    table |= {(last, j): blocks[last + j] for j in range(1, last + 1)}
    table[last, 0] = blocks[last].T
    for i in range(1, last):
        table[i, last] = blocks[last + i].T
    for i in range(last - 1):
        for j in range(last):
            factor = (SHIFTS[j] - SHIFTS[i]) / SCALE_POWER
            table[i + 1, j] = table[i, j + 1] + factor * table[i, j]
    return jnp.block([[table[i, j] for j in range(last + 1)] for i in range(last + 1)])


MESH = pl.DeviceIdType.MESH
ROWS = 5


def sum_everywhere(sides, x_ref, out_ref, plane, line, plane_sum, send_sem, plane_sem, line_sem):
    nz, ny, nx = sides
    gx, gy = lax.axis_index("gx"), lax.axis_index("gy")
    z, y, x, core = gx // ny, gx % ny, gy // 2, gy % 2

    def device(dz, dy, dx, dc):
        return ((z + dz) % nz * ny + (y + dy) % ny, (x + dx) % nx * 2 + (core + dc) % 2)

    planes = [(0, dy, dx, dc) for dy in range(ny) for dx in range(nx) for dc in range(2)][1:]
    lines = sorted([(dz, 0, 0, 0) for dz in range(1, nz)], key=lambda m: -min(m[0], nz - m[0]))
    barrier = pltpu.get_barrier_semaphore()
    for move in planes + lines:
        pl.semaphore_signal(barrier, inc=1, device_id=device(*move), device_id_type=MESH)
    pl.semaphore_wait(barrier, len(planes) + len(lines))

    def exchange(src, slots, moves, sem):
        def copy(k, move):
            return pltpu.make_async_remote_copy(
                src_ref=src.at[pl.ds(0, ROWS)],
                dst_ref=slots.at[k],
                send_sem=send_sem,
                recv_sem=sem,
                device_id=device(*move),
                device_id_type=MESH,
            )

        for k, move in enumerate(moves):
            copy(k, move).start()
        for end in (send_sem, sem):
            pltpu.make_async_copy(slots, slots, end).wait()

    exchange(x_ref, plane, planes, plane_sem)
    plane_sum[...] = x_ref[...] + jnp.sum(plane[...], axis=0)
    exchange(plane_sum, line, lines, line_sem)
    out_ref[...] = plane_sum[...] + jnp.sum(line[...], axis=0)


def all_reduce(words):
    ny = lax.axis_size("gx") // 32
    sides = (32, ny, lax.axis_size("gy") // 2)
    vmem = pl.BlockSpec(memory_space=pltpu.VMEM)
    return pl.pallas_call(
        functools.partial(sum_everywhere, sides),
        out_shape=jax.ShapeDtypeStruct((ROWS, 128), jnp.float32),
        in_specs=[vmem],
        out_specs=vmem,
        scratch_shapes=[
            pltpu.VMEM((sides[1] * sides[2] * 2 - 1, ROWS, 128), jnp.float32),
            pltpu.VMEM((sides[0] - 1, ROWS, 128), jnp.float32),
            pltpu.VMEM((ROWS, 128), jnp.float32),
            pltpu.SemaphoreType.DMA,
            pltpu.SemaphoreType.DMA,
            pltpu.SemaphoreType.DMA,
        ],
        compiler_params=pltpu.CompilerParams(collective_id=0, has_side_effects=True),
    )(words)


def apply_padded(padded, diag_inner, shift_now):
    along_z = jnp.pad(padded, ((0, 0), (0, 0), (0, 0), (1, 1)))
    sum_z = padded + WEIGHT_Z * (along_z[..., :-2] + along_z[..., 2:])
    sum_y = sum_z[:, :, 1:-1] + WEIGHT_Y * (sum_z[:, :, :-2] + sum_z[:, :, 2:])
    sum_x = sum_y[:, 1:-1] + WEIGHT_X * (sum_y[:, :-2] + sum_y[:, 2:])
    centre_cells = padded[:, 1:-1, 1:-1]
    return ((CENTRE + 1.0 + diag_inner - shift_now) * centre_cells - sum_x) / SCALE_POWER


def newton_table():
    blocks = len(SHIFTS)
    identity = np.eye(NRHS, dtype=np.float32)
    matrix = np.zeros(((blocks + 1) * NRHS, blocks * NRHS), np.float32)
    for block_index in range(blocks):
        low = block_index * NRHS
        matrix[low : low + NRHS, low : low + NRHS] = SHIFTS[block_index] * identity
        matrix[low + NRHS : low + 2 * NRHS, low : low + NRHS] = SCALE_POWER * identity
    return matrix


def solve_small(gram_full):
    highest = lax.Precision.HIGHEST
    newton = jnp.asarray(newton_table(), gram_full.dtype)
    image = jnp.dot(newton.T, jnp.dot(gram_full, newton, precision=highest), precision=highest)
    right_side = jnp.dot(newton.T, gram_full[:, :NRHS], precision=highest)
    scales = lax.rsqrt(jnp.diagonal(image) + EPSILON)
    scaled = image * scales[:, None] * scales[None, :]
    factor = jnp.linalg.cholesky(scaled)
    coeffs = scales[:, None] * jax.scipy.linalg.cho_solve(
        (factor, True), scales[:, None] * right_side
    )
    initial_sq = jnp.diagonal(gram_full)[:NRHS]
    estimate = (initial_sq - jnp.sum(right_side * coeffs, axis=0)) / initial_sq
    return (coeffs, jnp.dot(newton, coeffs, precision=highest), estimate)


def body(residual_block, diagonal):
    highest = lax.Precision.HIGHEST
    width_rhs, cells_x, cells_y, cells_z = residual_block.shape
    total_x = cells_x * lax.axis_size(GX)
    total_y = cells_y * lax.axis_size("gy")
    powers = [residual_block]
    depth = len(SHIFTS)
    outgoing = jnp.concatenate([residual_block, diagonal[None]], 0)
    extended = padded_2(outgoing, ((GX, 1), ("gy", 2)), depth)
    field_now = extended[:width_rhs]
    diag_wide = extended[width_rhs]
    coord_x = (
        lax.axis_index(GX) * cells_x - depth + jnp.arange(cells_x + 2 * depth, dtype=jnp.int32)
    )
    coord_y = (
        lax.axis_index("gy") * cells_y - depth + jnp.arange(cells_y + 2 * depth, dtype=jnp.int32)
    )
    inside_x = (coord_x >= 0) & (coord_x < total_x)
    inside_y = (coord_y >= 0) & (coord_y < total_y)
    for step_index, shift_now in enumerate(SHIFTS):
        margin = depth - 1 - step_index
        lower = depth - margin
        span_x = cells_x + 2 * margin
        span_y = cells_y + 2 * margin
        diag_now = diag_wide[lower : lower + span_x, lower : lower + span_y]
        field_now = apply_padded(field_now, diag_now, shift_now)
        inside = (
            inside_x[lower : lower + span_x][:, None] & inside_y[lower : lower + span_y][None, :]
        )
        field_now = jnp.where(inside[None, :, :, None], field_now, 0.0)
        powers.append(field_now[:, margin : margin + cells_x, margin : margin + cells_y])
    basis = jnp.concatenate(powers, 0).reshape(len(powers) * width_rhs, -1)
    local_gram = lax.dot_general(
        basis,
        basis,
        (((1,), (1,)), ((), ())),
        precision=highest,
        preferred_element_type=jnp.float32,
    )
    gram_full = from_moments(all_reduce(moments_of(local_gram)))
    coeffs, combined, estimate = solve_small(gram_full)
    kept = len(SHIFTS) * width_rhs
    correction = lax.dot_general(
        coeffs,
        basis[:kept],
        (((0,), (0,)), ((), ())),
        precision=highest,
        preferred_element_type=jnp.float32,
    )
    removed = lax.dot_general(
        combined,
        basis,
        (((0,), (0,)), ((), ())),
        precision=highest,
        preferred_element_type=jnp.float32,
    )
    new_residual = residual_block - removed.reshape(residual_block.shape)
    return (correction.reshape(residual_block.shape), new_residual, estimate)


def solution(mesh):
    placed = (P(None, GX, "gy", None), P(GX, "gy", None))
    return jax.shard_map(
        body,
        mesh=mesh,
        in_specs=placed,
        out_specs=(P(None, GX, "gy", None), P(None, GX, "gy", None), P()),
        check_vma=False,
    )
```

```python
import functools

import jax
import jax.numpy as jnp
from jax import lax
from jax.experimental import pallas as pl
from jax.experimental.pallas import tpu as pltpu
from jax.sharding import PartitionSpec as P

NRHS = 8
WEIGHT_X = 0.4
WEIGHT_Y = 0.2
WEIGHT_Z = 0.1
CENTRE = 2.2
SCALE_POWER = 3.0
SHIFTS = (6.0, 1.5, 4.5, 3.0)
DEPTH = len(SHIFTS)
BLOCKS = DEPTH + 1
MOMENTS = 2 * DEPTH + 1
ROWS = 4
LANES = 128
TILE = (8, LANES)
SPAN = 3 * DEPTH
MESH = pl.DeviceIdType.MESH
PLANE_SIDES = (4, 4)
VMEM_BYTES = 16 << 20


def iotas():
    return lax.broadcasted_iota(jnp.int32, TILE, 0), lax.broadcasted_iota(jnp.int32, TILE, 1)


def tiles_of(ref, *index):
    return [ref[(*index, slice(None), slice(h, h + LANES))] for h in (0, LANES)]


def next_plane(before, here, after, centre, factors, own_only):
    row, lane = iotas()
    first, last = row == 0, row == 7
    summed = [b + WEIGHT_X * (a + c) for a, b, c in zip(before, here, after)]
    down = [pltpu.roll(t, 1, 0) for t in summed]
    up = [pltpu.roll(t, 7, 0) for t in summed]
    out = []
    for tile in range(0, 2 if own_only else 4, 2):
        other = 2 - tile
        halves = []
        for h in (0, 1):
            low = jnp.where(first, down[other + h], down[tile + h])
            high = jnp.where(last, up[other + h], up[tile + h])
            halves.append(summed[tile + h] + WEIGHT_Y * (low + high))
        right = [pltpu.roll(t, 1, 1) for t in halves]
        left = [pltpu.roll(t, LANES - 1, 1) for t in halves]
        start, end = lane == 0, lane == LANES - 1
        low = [jnp.where(start, 0.0, right[0]), jnp.where(start, right[0], right[1])]
        high = [jnp.where(end, left[1], left[0]), jnp.where(end, 0.0, left[1])]
        for h in (0, 1):
            total = halves[h] + WEIGHT_Z * (low[h] + high[h])
            out.append(centre[tile + h] * here[tile + h] - factors[tile // 2] * total)
    return out


def moments_kernel(
    sides, residual, diagonal, basis, total, own, edge, centres, message, plane, line, plane_sum,
    load_sem, x_sem, y_sem, sent_x, sent_y, plane_sem, line_sem, sent_plane, sent_line, round_sem,
):
    nz, ny, nx = sides
    gx, gy = lax.axis_index("gx"), lax.axis_index("gy")
    z, y, x, core = gx // ny, gx % ny, gy // 2, gy % 2
    count_x, count_y = nz * ny, nx * 2

    def device(dz=0, dy=0, dx=0, dc=0):
        return ((z + dz) % nz * ny + (y + dy) % ny, (x + dx) % nx * 2 + (core + dc) % 2)

    def other(dz=0, dy=0, dx=0, dc=0):
        return bool(dz % nz or dy % ny or dx % nx or dc % 2)

    sides_x = [((gx - 1) % count_x, gy), ((gx + 1) % count_x, gy)]
    sides_y = [(gx, (gy - 1) % count_y), (gx, (gy + 1) % count_y)]

    for slot in range(NRHS + 1):
        source = residual.at[slot - 1] if slot else diagonal
        pltpu.make_async_copy(source, own.at[slot, pl.ds(DEPTH, DEPTH)], load_sem.at[slot]).start()

    barrier = pltpu.get_barrier_semaphore()
    near = sides_x + sides_y
    near += [device(**{axis: step}) for axis in ("dz", "dy", "dx") for step in (1, -1)]
    for one in near:
        pl.semaphore_signal(barrier, inc=1, device_id=one, device_id_type=MESH)
    message[...] = jnp.zeros(TILE, jnp.float32)
    pl.semaphore_wait(barrier, len(near))

    rounds = [
        [dict(dx=1), dict(dx=-1), dict(dy=1), dict(dy=-1), dict(dz=1), dict(dz=-1)],
        [dict(dx=1), dict(dx=-1), dict(dx=2), dict(dz=2), dict(dz=-2)],
        [dict(dc=1), dict(dz=4), dict(dz=-4)],
        [dict(dz=8), dict(dz=-8)],
    ]
    rounds = [[move for move in moves if other(**move)] for moves in rounds]

    def tell(n):
        for move in rounds[n]:
            pl.semaphore_signal(round_sem.at[n], inc=1, device_id=device(**move), device_id_type=MESH)

    def hear(n):
        if rounds[n]:
            pl.semaphore_wait(round_sem.at[n], len(rounds[n]))

    tell(0)

    def send_y(slot, planes):
        for near_y, half in zip(sides_y, (0, 4)):
            pltpu.make_async_remote_copy(
                src_ref=own.at[slot, planes, pl.ds(half, 4)],
                dst_ref=edge.at[slot, planes, pl.ds(half, 4)],
                send_sem=sent_y,
                recv_sem=y_sem.at[slot],
                device_id=near_y,
                device_id_type=MESH,
            ).start()

    def send_own(slot, _):
        here = own.at[slot, pl.ds(DEPTH, DEPTH)]
        pltpu.make_async_copy(here, here, load_sem.at[slot]).wait()
        for near_x, start in zip(sides_x, (2 * DEPTH, 0)):
            pltpu.make_async_remote_copy(
                src_ref=here,
                dst_ref=own.at[slot, pl.ds(start, DEPTH)],
                send_sem=sent_x,
                recv_sem=x_sem.at[slot],
                device_id=near_x,
                device_id_type=MESH,
            ).start()
        send_y(slot, pl.ds(DEPTH, DEPTH))
        return 0

    lax.fori_loop(0, NRHS + 1, send_own, 0)

    def pass_on(slot):
        both = own.at[slot, pl.ds(0, 2 * DEPTH)]
        pltpu.make_async_copy(both, both, x_sem.at[slot]).wait()
        send_y(slot, pl.ds(0, DEPTH))
        send_y(slot, pl.ds(2 * DEPTH, DEPTH))

    def whole(slot):
        pltpu.make_async_copy(edge.at[slot], edge.at[slot], y_sem.at[slot]).wait()

    row, lane = iotas()

    def flag(test):
        return jnp.where(test, 1.0, 0.0).astype(jnp.float32)

    around = jnp.where(row < 4, flag(gy < count_y - 1), flag(gy > 0))
    outside = {-1: flag(gx > 0), 0: jnp.float32(1.0), 1: flag(gx < count_x - 1)}

    def masks(plane_x, scale):
        side = outside[plane_x // DEPTH - 1] * scale
        return jnp.full(TILE, side, jnp.float32), around * side

    def prepare():
        for plane_x in range(1, SPAN - 1):
            tiles = tiles_of(own, 0, plane_x) + tiles_of(edge, 0, plane_x)
            for step, shift in enumerate(SHIFTS):
                if step < plane_x < SPAN - 1 - step:
                    for q, t in enumerate(tiles):
                        centres[step, plane_x, q] = (t + (CENTRE + 1.0 - shift)) * (1.0 / SCALE_POWER)

    def extend(slot):
        field = slot - 1
        levels = [{} for _ in range(BLOCKS)]
        for plane_x in range(SPAN):
            tiles = tiles_of(own, slot, plane_x) + tiles_of(edge, slot, plane_x)
            inner, outer = masks(plane_x, 1.0)
            if DEPTH <= plane_x < 2 * DEPTH:
                for h in (0, 1):
                    basis[0, field, plane_x - DEPTH, :, h * LANES : (h + 1) * LANES] = tiles[h]
            else:
                tiles[:2] = [t * inner for t in tiles[:2]]
            levels[0][plane_x] = tiles[:2] + [t * outer for t in tiles[2:]]
            for step in range(DEPTH):
                middle = plane_x - 1 - step
                if not step < middle < SPAN - 1 - step:
                    continue
                own_only = step == DEPTH - 1
                tiles = next_plane(
                    *(levels[step][middle + d] for d in (-1, 0, 1)),
                    [centres[step, middle, q] for q in range(2 if own_only else 4)],
                    masks(middle, 1.0 / SCALE_POWER),
                    own_only,
                )
                levels[step + 1][middle] = tiles
                if DEPTH <= middle < 2 * DEPTH:
                    for h in (0, 1):
                        basis[step + 1, field, middle - DEPTH, :, h * LANES : (h + 1) * LANES] = tiles[h]

    spots = [(plane_x, h) for plane_x in range(DEPTH) for h in (0, 1)]

    def at(power, field, spot):
        plane_x, h = spot
        return basis[power, field, plane_x, :, h * LANES : (h + 1) * LANES]

    def measure(slot):
        field = slot - 1
        zero = jnp.zeros(TILE, jnp.float32)

        def pair(e, columns):
            sums = [None] * MOMENTS
            for spot in spots:
                first, last = at(0, field, spot), at(DEPTH, field, spot)
                for power in range(BLOCKS):
                    value = at(power, e, spot)
                    terms = [(power, first * value)]
                    if power:
                        terms.append((DEPTH + power, last * value))
                    for k, term in terms:
                        sums[k] = term if sums[k] is None else sums[k] + term
            out = []
            for k in range(MOMENTS):
                s = sums[k]
                for step in (4, 2, 1):
                    s = s + pltpu.roll(s, step, 0)
                out.append(jnp.where(row == e, s, columns[k]))
            return tuple(out)

        columns = lax.fori_loop(0, field + 1, pair, (zero,) * MOMENTS)
        placed = zero
        for k in range(MOMENTS):
            column = jnp.broadcast_to(jnp.sum(columns[k], axis=1, keepdims=True), TILE)
            low = pltpu.roll(column, 4, 0)
            place = 72 + 8 * k + field if k < 7 else 72 + 8 * (k - 7) + field - 4
            place = jnp.where(field >= 4, place, -1)
            placed = placed + jnp.where((lane == 8 * k + field) & (row < 4), column, 0.0)
            placed = placed + jnp.where((lane == place) & (row < 4), low, 0.0)
        message[...] = message[...] + placed

    pass_on(0)
    pass_on(1)
    hear(0)
    tell(1)
    whole(0)
    prepare()

    def advance(slot, _):
        @pl.when(slot <= NRHS)
        def _():
            pass_on(slot)

        @pl.when(slot == 4)
        def _():
            hear(1)
            tell(2)

        @pl.when(slot == 7)
        def _():
            hear(2)
            tell(3)

        @pl.when(slot >= LAG + 1)
        def _():
            whole(slot - LAG)
            extend(slot - LAG)
            measure(slot - LAG)

        return 0

    lax.fori_loop(2, NRHS + 1 + LAG, advance, 0)

    def exchange(src, slots, moves, sent, sem):
        for k, move in enumerate(moves):
            pltpu.make_async_remote_copy(
                src_ref=src.at[pl.ds(0, ROWS)],
                dst_ref=slots.at[k],
                send_sem=sent,
                recv_sem=sem,
                device_id=device(*move),
                device_id_type=MESH,
            ).start()
        pltpu.make_async_copy(slots, slots, sem).wait()

    planes = [(0, dy, dx, dc) for dy in range(ny) for dx in range(nx) for dc in range(2)][1:]
    lines = sorted([(dz, 0, 0, 0) for dz in range(1, nz)], key=lambda m: -min(m[0], nz - m[0]))
    exchange(message, plane, planes, sent_plane, plane_sem)
    plane_sum[...] = message[: ROWS] + jnp.sum(plane[...], axis=0)
    hear(3)
    exchange(plane_sum, line, lines, sent_line, line_sem)
    total[: ROWS] = plane_sum[...] + jnp.sum(line[...], axis=0)
    total[ROWS:] = jnp.zeros((8 - ROWS, LANES), jnp.float32)

    for buffer, sem in ((own.at[:, pl.ds(0, 2 * DEPTH)], sent_x), (edge, sent_y), (plane, sent_plane), (line, sent_line)):
        pltpu.make_async_copy(buffer, buffer, sem).wait()


LAG = 3


def add_into(table, factor, terms):
    for k, value in terms.items():
        table[k] = table.get(k, 0.0) + factor * value


def expansions():
    gram = {}
    for j in range(BLOCKS):
        gram[0, j] = {j: 1.0}
        gram[DEPTH, j] = gram[j, DEPTH] = {DEPTH + j: 1.0}
    for i in range(DEPTH - 1):
        for j in range(DEPTH):
            gram[i + 1, j] = {}
            add_into(gram[i + 1, j], 1.0, gram[i, j + 1])
            add_into(gram[i + 1, j], (SHIFTS[j] - SHIFTS[i]) / SCALE_POWER, gram[i, j])
    image = {}
    for i in range(DEPTH):
        for j in range(DEPTH):
            image[i, j] = {}
            for a, left in ((i, SHIFTS[i]), (i + 1, SCALE_POWER)):
                for b, right in ((j, SHIFTS[j]), (j + 1, SCALE_POWER)):
                    add_into(image[i, j], left * right, gram[a, b])
    for i in range(DEPTH):
        image[i, DEPTH] = image[DEPTH, i] = {i: SHIFTS[i], i + 1: SCALE_POWER}
    return gram, image


def assemble(shifted, table, size):
    _, lane = iotas()
    block = lane // NRHS
    tiles = []
    for i in range(size):
        total = jnp.zeros(TILE, jnp.float32)
        places = [(j, k, value) for j in range(size) for k, value in table.get((i, j), {}).items() if value]
        for d in sorted({k - j for j, k, _ in places}):
            factor = jnp.zeros(TILE, jnp.float32)
            for j, k, value in places:
                if k - j == d:
                    factor = jnp.where(block == j, value, factor)
            total = total + factor * shifted[d]
        tiles.append(total)
    return tiles


def plus_transpose(tiles):
    whole = jnp.concatenate(tiles + [jnp.zeros((LANES - 8 * len(tiles), LANES), jnp.float32)], 0)
    turned = jnp.transpose(whole)
    return [t + turned[8 * b : 8 * b + 8] for b, t in enumerate(tiles)]


def lane_of(tile, index):
    return jnp.broadcast_to(tile[:, index : index + 1], TILE)


def row_of(tile, index):
    return jnp.broadcast_to(tile[index : index + 1, :], TILE)


def eliminate(tiles):
    row, _ = iotas()
    tiles = list(tiles)
    for p in range(DEPTH):
        columns = [[lane_of(t, NRHS * p + c) for t in tiles] for c in range(NRHS)]
        for c in range(NRHS):
            pivot = 1.0 / row_of(columns[c][p], c)
            factor = [t * pivot for t in columns[c]]

            def step(rows):
                pivot_row = row_of(rows[p], c)
                out = [t - f * pivot_row for t, f in zip(rows, factor)]
                out[p] = jnp.where(row == c, pivot_row * pivot, out[p])
                return out

            for later in range(c + 1, NRHS):
                columns[later] = step(columns[later])
            tiles = step(tiles)
    return tiles


def combine_kernel(total, basis, correction, new_residual, estimate, weights, results, sem):
    row, lane = iotas()
    words = total[...]
    low = jnp.where(lane < 56, pltpu.roll(words, 56, 1), pltpu.roll(words, 116, 1))
    moments = jnp.where(row < 4, words, pltpu.roll(low, 4, 0))
    place = lane % NRHS
    half = jnp.where(row == place, 0.5, 1.0)
    moments = jnp.where((row <= place) & (lane < MOMENTS * NRHS), half * moments, 0.0)
    shifted = {d: pltpu.roll(moments, -NRHS * d % LANES, 1) for d in range(-DEPTH, MOMENTS)}
    gram_table, image_table = expansions()
    tiles = plus_transpose(assemble(shifted, image_table, BLOCKS))[:DEPTH]
    coeffs = eliminate(tiles)
    first = NRHS * DEPTH
    inside = (lane >= first) & (lane < first + NRHS)
    unit = jnp.where(lane == row + first, 1.0, 0.0)
    kept = []
    for j in range(BLOCKS):
        value = unit if j == 0 else jnp.zeros(TILE, jnp.float32)
        if j < DEPTH:
            value = value - SHIFTS[j] * coeffs[j]
        if j:
            value = value - SCALE_POWER * coeffs[j - 1]
        kept.append(jnp.where(inside, value, 0.0))
    for r in range(NRHS):
        for k, tile in enumerate(coeffs + kept):
            weights[r, k] = lane_of(tile, first + r)

    gram = plus_transpose(assemble(shifted, gram_table, BLOCKS))
    size = BLOCKS * NRHS
    side = jnp.concatenate(kept, 0)
    product = jnp.dot(
        jnp.concatenate(gram, 0)[:, :size], side, precision=lax.Precision.HIGHEST, preferred_element_type=jnp.float32
    )
    left_over = jnp.sum(side * product, axis=0, keepdims=True)
    start = jnp.sum(jnp.where(row == lane, gram[0], 0.0), axis=0, keepdims=True)
    estimate[...] = left_over[:, first : first + NRHS] / start[:, :NRHS]

    spots = [(plane_x, h) for plane_x in range(DEPTH) for h in (0, 1)]

    def at(ref, spot, *index):
        plane_x, h = spot
        return ref.at[(*index, plane_x, slice(None), pl.ds(h * LANES, LANES))]

    def field(r, _):
        sums = [[jnp.zeros(TILE, jnp.float32)] * len(spots) for _ in range(2)]
        for j in range(BLOCKS):
            for e in range(NRHS):
                values = [at(basis, spot, j, e)[...] for spot in spots]
                for n in (0, 1):
                    if n == 0 and j == DEPTH:
                        continue
                    factor = jnp.broadcast_to(weights[r, n * DEPTH + j, e : e + 1, :], TILE)
                    sums[n] = [s + factor * v for s, v in zip(sums[n], values)]
        for n, out in enumerate((correction, new_residual)):
            for spot, s in zip(spots, sums[n]):
                at(results, spot, n, r)[...] = s
            pltpu.make_async_copy(results.at[n, r], out.at[r], sem).start()
        return 0

    lax.fori_loop(0, NRHS, field, 0)
    pltpu.make_async_copy(results, results, sem).wait()


def solution(mesh, plane_sides=PLANE_SIDES):
    ny, nx = plane_sides
    sides = (mesh.shape["gx"] // ny, ny, nx)
    vmem, hbm = pl.BlockSpec(memory_space=pltpu.VMEM), pl.BlockSpec(memory_space=pltpu.HBM)
    f32 = jnp.float32

    def body(residual, diagonal):
        cells = residual.shape[1:]
        extended = (NRHS + 1, SPAN, *cells[1:])
        dma = pltpu.SemaphoreType.DMA
        basis, total = pl.pallas_call(
            functools.partial(moments_kernel, sides),
            name="moments",
            out_shape=(
                jax.ShapeDtypeStruct((BLOCKS, *residual.shape), f32),
                jax.ShapeDtypeStruct(TILE, f32),
            ),
            in_specs=[hbm, hbm],
            out_specs=(vmem, vmem),
            scratch_shapes=[
                pltpu.VMEM(extended, f32),
                pltpu.VMEM(extended, f32),
                pltpu.VMEM((DEPTH, SPAN, 4, *TILE), f32),
                pltpu.VMEM(TILE, f32),
                pltpu.VMEM((ny * nx * 2 - 1, ROWS, LANES), f32),
                pltpu.VMEM((sides[0] - 1, ROWS, LANES), f32),
                pltpu.VMEM((ROWS, LANES), f32),
                dma((NRHS + 1,)),
                dma((NRHS + 1,)),
                dma((NRHS + 1,)),
                dma,
                dma,
                dma,
                dma,
                dma,
                dma,
                pltpu.SemaphoreType.REGULAR((4,)),
            ],
            compiler_params=pltpu.CompilerParams(collective_id=0, has_side_effects=True, vmem_limit_bytes=VMEM_BYTES),
        )(residual, diagonal)
        correction, new_residual, estimate = pl.pallas_call(
            combine_kernel,
            name="combine",
            out_shape=(
                jax.ShapeDtypeStruct(residual.shape, f32),
                jax.ShapeDtypeStruct(residual.shape, f32),
                jax.ShapeDtypeStruct((1, NRHS), f32),
            ),
            in_specs=[vmem, vmem],
            out_specs=(hbm, hbm, vmem),
            scratch_shapes=[
                pltpu.VMEM((NRHS, DEPTH + BLOCKS, *TILE), f32),
                pltpu.VMEM((2, *residual.shape), f32),
                dma,
            ],
            compiler_params=pltpu.CompilerParams(vmem_limit_bytes=VMEM_BYTES),
        )(total, basis)
        return correction, new_residual, estimate.reshape(NRHS)

    placed = P(None, "gx", "gy", None)
    return jax.shard_map(
        body,
        mesh=mesh,
        in_specs=(placed, P("gx", "gy", None)),
        out_specs=(placed, placed, P()),
        check_vma=False,
    )
```
